128 devices in a mesh: pod: 1, dp: 2 (over core), sp: 64 (over z, y, x).
Axes of the slice: x: 4, y: 4, z: 4, core: 2. Of those that a mesh axis runs over, the one named last changes fastest.
Arguments:
- x: bfloat16 [24, 128, 64, 1024], P(('pod', 'dp'), 'sp')
- norm_gain: bfloat16 [2, 2, 1024], replicated
- norm_shift: bfloat16 [2, 2, 1024], replicated
- w_qkv: bfloat16 [2, 3, 1024, 16, 64], replicated
- w_out: bfloat16 [2, 16, 64, 1024], replicated
- w_up: bfloat16 [2, 1024, 4096], replicated
- w_down: bfloat16 [2, 4096, 1024], replicated
Outputs:
- output: bfloat16 [24, 128, 64, 1024], P(('pod', 'dp'), 'sp')
All inputs are finite; a program needn't handle non-finite values.
Results may differ from the reference program's by a relative error of at most 0.0154772.
Values are sent between devices in bfloat16 or wider.
A program may use at most 1 GiB of HBM per device.

```python
import jax
import jax.numpy as jnp
from jax import lax

NUM_VIDEOS = 24
NUM_FRAMES = 128
NUM_PATCHES = 64
MODEL_WIDTH = 1024
NUM_HEADS = 16

HEAD_DIM = MODEL_WIDTH // NUM_HEADS
FF_WIDTH = 4 * MODEL_WIDTH
LN_EPS = 1e-6
QK_GAIN = 1.5


def layer_norm(tokens, gain, shift):
    tok_f = tokens.astype(jnp.float32)
    mean_val = jnp.mean(tok_f, axis=-1, keepdims=True)
    centered = tok_f - mean_val
    var_val = jnp.mean(centered * centered, axis=-1, keepdims=True)
    normed = centered * lax.rsqrt(var_val + LN_EPS)
    return (normed * gain.astype(jnp.float32) + shift.astype(jnp.float32)).astype(jnp.bfloat16)


def seq_block(tokens, gains, shifts, w_qkv, w_out, w_up, w_down):
    normed = layer_norm(tokens, gains[0], shifts[0])
    proj_qkv = jnp.einsum('ld,kdhe->klhe', normed.astype(jnp.float32), w_qkv.astype(jnp.float32)).astype(jnp.bfloat16)
    scores = jnp.einsum('lhe,mhe->hlm', proj_qkv[0].astype(jnp.float32), proj_qkv[1].astype(jnp.float32)) * (HEAD_DIM ** -0.5)
    attn_probs = jax.nn.softmax(scores, axis=-1).astype(jnp.bfloat16)
    mixed = jnp.einsum('hlm,mhe->lhe', attn_probs.astype(jnp.float32), proj_qkv[2].astype(jnp.float32)).astype(jnp.bfloat16)
    attn_proj = jnp.einsum('lhe,hed->ld', mixed.astype(jnp.float32), w_out.astype(jnp.float32)).astype(jnp.bfloat16)
    hidden = (tokens.astype(jnp.float32) + attn_proj.astype(jnp.float32)).astype(jnp.bfloat16)
    normed_mlp = layer_norm(hidden, gains[1], shifts[1])
    up_proj = jnp.dot(normed_mlp, w_up, preferred_element_type=jnp.float32).astype(jnp.bfloat16)
    activated = jax.nn.gelu(up_proj.astype(jnp.float32), approximate=True).astype(jnp.bfloat16)
    down_proj = jnp.dot(activated, w_down, preferred_element_type=jnp.float32).astype(jnp.bfloat16)
    return (hidden.astype(jnp.float32) + down_proj.astype(jnp.float32)).astype(jnp.bfloat16)


def setup_inputs(seed: int = 0, part: int = 0) -> dict:
    base_key = jax.random.key(seed)
    key_list = jax.random.split(base_key, 7)
    data_key = jax.random.fold_in(key_list[0], part)
    key_frame, key_patch, key_noise = jax.random.split(data_key, 3)
    frame_code = jax.random.normal(key_frame, (NUM_VIDEOS, NUM_FRAMES, 1, MODEL_WIDTH), jnp.float32)
    patch_code = jax.random.normal(key_patch, (NUM_VIDEOS, 1, NUM_PATCHES, MODEL_WIDTH), jnp.float32)
    noise_val = jax.random.normal(key_noise, (NUM_VIDEOS, NUM_FRAMES, NUM_PATCHES, MODEL_WIDTH), jnp.float32)
    x = (frame_code + patch_code + 0.5 * noise_val).astype(jnp.bfloat16)
    norm_gain = (1.0 + 0.4 * jax.random.normal(key_list[1], (2, 2, MODEL_WIDTH), jnp.float32)).astype(jnp.bfloat16)
    norm_shift = (0.4 * jax.random.normal(key_list[2], (2, 2, MODEL_WIDTH), jnp.float32)).astype(jnp.bfloat16)
    qkv_gain = jnp.array([QK_GAIN, QK_GAIN, 1.0], jnp.float32).reshape(1, 3, 1, 1, 1)
    w_qkv = (jax.random.normal(key_list[3], (2, 3, MODEL_WIDTH, NUM_HEADS, HEAD_DIM), jnp.float32) * (MODEL_WIDTH ** -0.5) * qkv_gain).astype(jnp.bfloat16)
    w_out = (jax.random.normal(key_list[4], (2, NUM_HEADS, HEAD_DIM, MODEL_WIDTH), jnp.float32) * (MODEL_WIDTH ** -0.5)).astype(jnp.bfloat16)
    w_up = (jax.random.normal(key_list[5], (2, MODEL_WIDTH, FF_WIDTH), jnp.float32) * (MODEL_WIDTH ** -0.5)).astype(jnp.bfloat16)
    w_down = (jax.random.normal(key_list[6], (2, FF_WIDTH, MODEL_WIDTH), jnp.float32) * (FF_WIDTH ** -0.5)).astype(jnp.bfloat16)
    return {'x': x, 'norm_gain': norm_gain, 'norm_shift': norm_shift, 'w_qkv': w_qkv, 'w_out': w_out, 'w_up': w_up, 'w_down': w_down}


def reference(x, norm_gain, norm_shift, w_qkv, w_out, w_up, w_down):
    num_videos, num_frames, num_patches, model_width = x.shape

    def spatial_fn(frame_tok):
        return seq_block(frame_tok, norm_gain[0], norm_shift[0], w_qkv[0], w_out[0], w_up[0], w_down[0])

    def temporal_fn(tube_tok):
        return seq_block(tube_tok, norm_gain[1], norm_shift[1], w_qkv[1], w_out[1], w_up[1], w_down[1])

    frame_rows = x.reshape(num_videos * num_frames, num_patches, model_width)
    spatial_out = lax.map(spatial_fn, frame_rows).reshape(num_videos, num_frames, num_patches, model_width)
    tube_rows = jnp.transpose(spatial_out, (0, 2, 1, 3)).reshape(num_videos * num_patches, num_frames, model_width)
    temporal_out = lax.map(temporal_fn, tube_rows).reshape(num_videos, num_patches, num_frames, model_width)
    return jnp.transpose(temporal_out, (0, 2, 1, 3))
```

```python
import jax
import jax.numpy as jnp
from jax import lax
from jax.experimental import pallas as pl
from jax.experimental.pallas import tpu as pltpu
from jax.sharding import PartitionSpec as P

LN_EPS = 1e-6
F32 = jnp.float32
BF16 = jnp.bfloat16
D = 1024
FF = 4096
RANKS = 64
GROUPS = 3
ROWS = 8
TILE = 256
HALF = 512
SEND_STEP = 23
MESH = pl.DeviceIdType.MESH


def dot_nt(a, b):
    return lax.dot_general(a, b, (((1,), (1,)), ((), ())), preferred_element_type=F32)


def dot(a, b):
    return jnp.dot(a, b, preferred_element_type=F32)


def normalize(tok, gain, shift):
    mean = jnp.mean(tok, axis=-1, keepdims=True)
    cen = tok - mean
    var = jnp.mean(cen * cen, axis=-1, keepdims=True)
    return cen * lax.rsqrt(var + LN_EPS) * gain + shift


def kernel(x_hbm, ng_ref, ns_ref, wqkv_hbm, wo_hbm, wu_hbm, wd_hbm, y_hbm,
           wq0, wq1, wo, wu, wd, xb, yb, t_buf, i_buf, os_buf, or_buf,
           n_buf, qkv, o_buf, r_buf, g_buf, stage, gain, shift, bd_s, bd_t,
           wsem, xsem, ysem, lsem, ssem, rsem):
    me = lax.axis_index("sp")

    def weight_copies(j):
        return (
            pltpu.make_async_copy(wo_hbm.at[j], wo, wsem.at[2]),
            pltpu.make_async_copy(wu_hbm.at[j], wu, wsem.at[3]),
            pltpu.make_async_copy(wd_hbm.at[j], wd, wsem.at[4]),
        )

    def x_copy(i):
        return pltpu.make_async_copy(x_hbm.at[pl.ds(2 * i, 2)], xb.at[lax.rem(i, 2)], xsem.at[lax.rem(i, 2)])

    def y_copy(i):
        c, half = i // 2, lax.rem(i, 2)
        dst = y_hbm.at[pl.ds(4 * c, 4), :, pl.ds(pl.multiple_of(32 * half, 32), 32), :]
        return pltpu.make_async_copy(yb.at[half], dst, ysem.at[half])

    wq0_copy = pltpu.make_async_copy(wqkv_hbm.at[0], wq0, wsem.at[0])
    wq1_copy = pltpu.make_async_copy(wqkv_hbm.at[1], wq1, wsem.at[1])
    x_copy(0).start()
    wq0_copy.start()
    for copy in weight_copies(0):
        copy.start()
    wq1_copy.start()
    barrier = pltpu.get_barrier_semaphore()

    @pl.loop(1, RANKS)
    def _(i):
        pl.semaphore_signal(barrier, 1, device_id={"sp": lax.rem(me + i, RANKS)}, device_id_type=MESH)

    gain[...] = ng_ref[...].astype(F32)
    shift[...] = ns_ref[...].astype(F32)
    row = lax.broadcasted_iota(jnp.int32, (256, 256), 0)
    col = lax.broadcasted_iota(jnp.int32, (256, 256), 1)
    bd_s[...] = jnp.where(row // 64 == col // 64, 1.0, 0.0).astype(BF16)
    row = lax.broadcasted_iota(jnp.int32, (256, 128), 0)
    col = lax.broadcasted_iota(jnp.int32, (256, 128), 1)
    bd_t[...] = jnp.where(row // 128 == col // 64, 1.0, 0.0).astype(BF16)
    pl.semaphore_wait(barrier, RANKS - 1)

    def exchange(src, dst, c, k):
        pltpu.make_async_copy(src.at[c, me], dst.at[c, me], lsem.at[k, c]).start()

        @pl.loop(1, RANKS)
        def _(i):
            peer = lax.rem(me + lax.rem(i * SEND_STEP, RANKS), RANKS)
            pltpu.make_async_remote_copy(
                src_ref=src.at[c, peer], dst_ref=dst.at[c, me], send_sem=ssem.at[k, c], recv_sem=rsem.at[k, c],
                device_id={"sp": peer}, device_id_type=MESH).start()

    def arrived(dst, c, k):
        pltpu.make_async_copy(dst.at[c, 0], dst.at[c, 0], lsem.at[k, c]).wait()
        blocks = dst.at[c, pl.ds(0, RANKS - 1)]
        pltpu.make_async_copy(blocks, blocks, rsem.at[k, c]).wait()

    def stage_get(first, count, step):
        return jnp.concatenate([stage[b, pl.ds(first, count, stride=step), :] for b in range(8)], axis=1).astype(BF16)

    def stage_put(rows, first, value):
        for b in range(value.shape[1] // 128):
            stage[first + b, rows, :] = value[:, b * 128:b * 128 + 128]

    def regroup(dst, c):
        @pl.loop(0, RANKS, unroll=4)
        def _(p):
            dst[c, p] = stage_get(p, ROWS, RANKS)

    def spatial_attention():
        low = lax.broadcasted_iota(jnp.int32, (64, 128), 1) < 64

        @pl.loop(0, 4)
        def _(f):
            rows = pl.ds(pl.multiple_of(f * 64, 64), 64)
            bd = bd_s[...]
            for quad in range(4):
                c0 = quad * 256
                q = qkv[rows, c0:c0 + 256]
                k = qkv[rows, D + c0:D + c0 + 256]
                v = qkv[rows, 2 * D + c0:2 * D + c0 + 256]
                kb = jnp.concatenate([k, k, k, k], axis=0) * bd
                vb = jnp.concatenate([v, v, v, v], axis=0) * bd
                s = dot_nt(q, kb)
                parts = []
                for side in range(2):
                    sc = s[:, side * 128:side * 128 + 128]
                    m0 = jnp.max(jnp.where(low, sc, -jnp.inf), axis=-1, keepdims=True)
                    m1 = jnp.max(jnp.where(low, -jnp.inf, sc), axis=-1, keepdims=True)
                    e = jnp.exp((sc - jnp.where(low, m0, m1)) * 0.125)
                    d0 = jnp.sum(jnp.where(low, e, 0.0), axis=-1, keepdims=True)
                    d1 = jnp.sum(jnp.where(low, 0.0, e), axis=-1, keepdims=True)
                    parts.append((e * jnp.where(low, 1.0 / d0, 1.0 / d1)).astype(BF16))
                o_buf[rows, c0:c0 + 256] = dot(jnp.concatenate(parts, axis=1), vb).astype(BF16)

    def temporal_attention():
        @pl.loop(0, 4)
        def _(vid):
            rows = pl.ds(pl.multiple_of(vid * 128, 128), 128)
            bd = bd_t[...]
            for pair in range(8):
                c0 = pair * 128
                q = qkv[rows, c0:c0 + 128]
                k = qkv[rows, D + c0:D + c0 + 128]
                v = qkv[rows, 2 * D + c0:2 * D + c0 + 128]
                kb = jnp.concatenate([k, k], axis=0) * bd
                vb = jnp.concatenate([v, v], axis=0) * bd
                s = dot_nt(q, kb)
                parts = []
                for side in range(2):
                    sc = s[:, side * 128:side * 128 + 128]
                    e = jnp.exp((sc - jnp.max(sc, axis=-1, keepdims=True)) * 0.125)
                    parts.append((e * (1.0 / jnp.sum(e, axis=-1, keepdims=True))).astype(BF16))
                stage[pair, rows, :] = dot(jnp.concatenate(parts, axis=1), vb).astype(BF16).astype(F32)

    def spatial_front(i):
        slot = lax.rem(i, 2)
        x_copy(i).wait()

        @pl.when(i + 1 < 2 * GROUPS)
        def _():
            x_copy(i + 1).start()

        g1, s1 = gain[0, 0:1, :], shift[0, 0:1, :]

        @pl.loop(0, 4)
        def _(b):
            rows = pl.ds(pl.multiple_of(b * 64, 64), 64)
            tok = xb[slot, b // 2, lax.rem(b, 2)]
            r_buf[rows, :] = tok
            n_buf[rows, :] = normalize(tok.astype(F32), g1, s1).astype(BF16)

        @pl.when(i == 0)
        def _():
            wq0_copy.wait()

        @pl.loop(0, 6)
        def _(j):
            cols = pl.ds(pl.multiple_of(j * 512, 512), 512)
            qkv[0:TILE, cols] = dot_nt(n_buf[0:TILE, :], wq0[cols, :]).astype(BF16)

        spatial_attention()

    def tail_front(i):
        c, half = i // 2, lax.rem(i, 2)

        @pl.when(half == 0)
        def _():
            arrived(or_buf, c, 1)

        @pl.loop(0, 4)
        def _(b):
            rows = pl.ds(pl.multiple_of(b * 64, 64), 64)
            peers = pl.ds(half * 32 + b * 8, 8)
            r_buf[rows, :] = t_buf[c, peers].astype(F32).reshape(64, D).astype(BF16)
            o_buf[rows, :] = or_buf[c, peers].astype(F32).reshape(64, D).astype(BF16)

    def tail(j, base):
        for col in range(2):
            cols = slice(col * 512, col * 512 + 512)
            a = dot(o_buf[...], wo[:, cols]).astype(BF16)
            r_buf[:, cols] = (r_buf[:, cols].astype(F32) + a.astype(F32)).astype(BF16)
        g2, s2 = gain[j, 1:2, :], shift[j, 1:2, :]

        @pl.loop(0, 4)
        def _(b):
            rows = pl.ds(pl.multiple_of(b * 64, 64), 64)
            n_buf[rows, :] = normalize(r_buf[rows, :].astype(F32), g2, s2).astype(BF16)

        @pl.loop(0, 8)
        def _(k):
            cols = pl.ds(pl.multiple_of(k * 512, 512), 512)
            u = dot(n_buf[0:TILE, :], wu[:, cols]).astype(BF16)
            g_buf[:, cols] = jax.nn.gelu(u.astype(F32), approximate=True).astype(BF16)

        @pl.loop(0, 4)
        def _(k):
            cols = pl.ds(pl.multiple_of(k * 256, 256), 256)
            m = dot(g_buf[...], wd[:, cols]).astype(BF16)
            out = (r_buf[:, cols].astype(F32) + m.astype(F32)).astype(BF16)
            stage_put(pl.ds(base, TILE), 2 * k, out.astype(F32))

    def temporal(c):
        arrived(i_buf, c, 0)
        g1, s1 = gain[1, 0:1, :], shift[1, 0:1, :]

        @pl.loop(0, 8)
        def _(b):
            rows = pl.ds(pl.multiple_of(b * 64, 64), 64)
            tok = i_buf[c, pl.ds(b * 8, 8)].astype(F32).reshape(64, D)
            stage_put(rows, 0, normalize(tok, g1, s1))

        for r in range(ROWS):
            n_buf[r * 64:(r + 1) * 64, :] = stage_get(r, RANKS, ROWS)

        @pl.when(c == 0)
        def _():
            wq1_copy.wait()

        @pl.loop(0, 12)
        def _(j):
            cols = pl.ds(pl.multiple_of(j * 256, 256), 256)
            qkv[:, cols] = dot_nt(n_buf[...], wq1[cols, :]).astype(BF16)

        temporal_attention()
        regroup(os_buf, c)
        exchange(os_buf, or_buf, c, 1)

    def tail_back(i):
        half = lax.rem(i, 2)

        @pl.when(i >= 2)
        def _():
            y_copy(i - 2).wait()

        for r in range(ROWS):
            yb[half, r // 2, r % 2] = stage_get(r, 32, ROWS)
        y_copy(i).start()

    @pl.loop(0, 2 * GROUPS)
    def _(step):
        spatial = step < GROUPS

        @pl.loop(0, 2)
        def _(half):
            i = 2 * step + half

            @pl.when(spatial)
            def _():
                spatial_front(i)

            @pl.when(step >= GROUPS)
            def _():
                tail_front(i - 2 * GROUPS)

            @pl.when(jnp.logical_and(half == 0, jnp.logical_or(step == 0, step == GROUPS)))
            def _():
                for copy in weight_copies(0):
                    copy.wait()

            tail(jnp.where(spatial, 0, 1), pl.multiple_of(jnp.where(spatial, half * TILE, 0), TILE))

            @pl.when(step >= GROUPS)
            def _():
                tail_back(i - 2 * GROUPS)

        @pl.when(step == GROUPS - 1)
        def _():
            for copy in weight_copies(1):
                copy.start()

        @pl.when(spatial)
        def _():
            regroup(t_buf, step)
            exchange(t_buf, i_buf, step, 0)

        @pl.when(jnp.logical_and(step >= 1, step <= GROUPS))
        def _():
            temporal(step - 1)

    y_copy(2 * GROUPS - 2).wait()
    y_copy(2 * GROUPS - 1).wait()
    for k, buf in enumerate((t_buf, os_buf)):
        for c in range(GROUPS):
            blocks = buf.at[c, pl.ds(0, RANKS - 1)]
            pltpu.make_async_copy(blocks, blocks, ssem.at[k, c]).wait()


def solution(mesh):
    tok_spec = P(('pod', 'dp'), 'sp', None, None)
    hbm = pl.BlockSpec(memory_space=pl.ANY)
    vmem = pl.BlockSpec(memory_space=pltpu.VMEM)
    comm = pltpu.VMEM((GROUPS, RANKS, ROWS, D), BF16)

    call = pl.pallas_call(
        kernel,
        out_shape=jax.ShapeDtypeStruct((12, 2, 64, D), BF16),
        in_specs=[hbm, vmem, vmem, hbm, hbm, hbm, hbm],
        out_specs=hbm,
        scratch_shapes=[
            pltpu.VMEM((3 * D, D), BF16), pltpu.VMEM((3 * D, D), BF16),
            pltpu.VMEM((D, D), BF16), pltpu.VMEM((D, FF), BF16), pltpu.VMEM((FF, D), BF16),
            pltpu.VMEM((2, 2, 2, 64, D), BF16), pltpu.VMEM((2, 4, 2, 32, D), BF16),
            comm, comm, comm, comm,
            pltpu.VMEM((HALF, D), BF16), pltpu.VMEM((HALF, 3 * D), BF16), pltpu.VMEM((TILE, D), BF16),
            pltpu.VMEM((TILE, D), BF16), pltpu.VMEM((TILE, FF), BF16), pltpu.VMEM((8, HALF, 128), F32),
            pltpu.VMEM((2, 2, D), F32), pltpu.VMEM((2, 2, D), F32),
            pltpu.VMEM((256, 256), BF16), pltpu.VMEM((256, 128), BF16),
            pltpu.SemaphoreType.DMA((5,)), pltpu.SemaphoreType.DMA((2,)), pltpu.SemaphoreType.DMA((2,)),
            pltpu.SemaphoreType.DMA((2, GROUPS)), pltpu.SemaphoreType.DMA((2, GROUPS)),
            pltpu.SemaphoreType.DMA((2, GROUPS)),
        ],
        compiler_params=pltpu.CompilerParams(
            collective_id=0, has_side_effects=True, vmem_limit_bytes=66 * 1000 * 1000),
    )

    def local_step(x_loc, norm_gain, norm_shift, w_qkv, w_out, w_up, w_down):
        w_t = jnp.transpose(w_qkv, (0, 1, 3, 4, 2)).reshape(2, 3 * D, D)
        return call(x_loc, norm_gain, norm_shift, w_t, w_out.reshape(2, D, D), w_up, w_down)

    return jax.shard_map(local_step, mesh=mesh, in_specs=(tok_spec, P(), P(), P(), P(), P(), P()), out_specs=tok_spec, check_vma=False)
```

```python
import jax
import jax.numpy as jnp
from jax import lax
from jax.experimental import pallas as pl
from jax.experimental.pallas import tpu as pltpu
from jax.sharding import PartitionSpec as P

LN_EPS = 1e-6
F32 = jnp.float32
BF16 = jnp.bfloat16
D = 1024
FF = 4096
RANKS = 64
GROUPS = 3
ROWS = 8
TILE = 256
HALF = 512
SEND_STEP = 23
EXP_SCALE = 0.125 * 1.4426950408889634
GELU_A = 0.7978845608028654
GELU_B = GELU_A * 0.044715
MESH = pl.DeviceIdType.MESH


def dot_nt(a, b):
    return lax.dot_general(a, b, (((1,), (1,)), ((), ())), preferred_element_type=F32)


def dot(a, b):
    return jnp.dot(a, b, preferred_element_type=F32)


def gelu(u):
    half = 0.5 * u
    return half + half * jnp.tanh(u * (GELU_A + GELU_B * (u * u)))


def normalize(tok, gain, shift):
    mean = jnp.mean(tok, axis=-1, keepdims=True)
    cen = tok - mean
    var = jnp.mean(cen * cen, axis=-1, keepdims=True)
    return cen * lax.rsqrt(var + LN_EPS) * gain + shift


def kernel(x_hbm, ng_ref, ns_ref, wqkv_hbm, wo_hbm, wu_hbm, wd_hbm, y_hbm,
           wq0, wq1, wo, wu, wd, xb, yb, t_buf, i_buf, os_buf, or_buf,
           n_buf, qkv, o_buf, r_buf, g_buf, stage, gain, shift, bd_s, bd_t,
           wsem, xsem, ysem, lsem, ssem, rsem):
    me = lax.axis_index("sp")

    def weight_copies(j):
        return (
            pltpu.make_async_copy(wo_hbm.at[j], wo, wsem.at[2]),
            pltpu.make_async_copy(wu_hbm.at[j], wu, wsem.at[3]),
            pltpu.make_async_copy(wd_hbm.at[j], wd, wsem.at[4]),
        )

    def x_copy(i):
        return pltpu.make_async_copy(x_hbm.at[pl.ds(2 * i, 2)], xb.at[lax.rem(i, 2)], xsem.at[lax.rem(i, 2)])

    def y_copy(i):
        c, half = i // 2, lax.rem(i, 2)
        dst = y_hbm.at[pl.ds(4 * c, 4), :, pl.ds(pl.multiple_of(32 * half, 32), 32), :]
        return pltpu.make_async_copy(yb.at[half], dst, ysem.at[half])

    wq0_copy = pltpu.make_async_copy(wqkv_hbm.at[0], wq0, wsem.at[0])
    wq1_copy = pltpu.make_async_copy(wqkv_hbm.at[1], wq1, wsem.at[1])
    x_copy(0).start()
    wq0_copy.start()
    for copy in weight_copies(0):
        copy.start()
    wq1_copy.start()
    barrier = pltpu.get_barrier_semaphore()

    @pl.loop(1, RANKS)
    def _(i):
        pl.semaphore_signal(barrier, 1, device_id={"sp": lax.rem(me + i, RANKS)}, device_id_type=MESH)

    gain[...] = ng_ref[...].astype(F32)
    shift[...] = ns_ref[...].astype(F32)
    row = lax.broadcasted_iota(jnp.int32, (256, 256), 0)
    col = lax.broadcasted_iota(jnp.int32, (256, 256), 1)
    bd_s[...] = jnp.where(row // 64 == col // 64, 1.0, 0.0).astype(BF16)
    row = lax.broadcasted_iota(jnp.int32, (256, 128), 0)
    col = lax.broadcasted_iota(jnp.int32, (256, 128), 1)
    bd_t[...] = jnp.where(row // 128 == col // 64, 1.0, 0.0).astype(BF16)
    pl.semaphore_wait(barrier, RANKS - 1)

    def exchange(src, dst, c, k):
        pltpu.make_async_copy(src.at[c, me], dst.at[c, me], lsem.at[k, c]).start()

        @pl.loop(1, RANKS)
        def _(i):
            peer = lax.rem(me + lax.rem(i * SEND_STEP, RANKS), RANKS)
            pltpu.make_async_remote_copy(
                src_ref=src.at[c, peer], dst_ref=dst.at[c, me], send_sem=ssem.at[k, c], recv_sem=rsem.at[k, c],
                device_id={"sp": peer}, device_id_type=MESH).start()

    def arrived(dst, c, k):
        pltpu.make_async_copy(dst.at[c, 0], dst.at[c, 0], lsem.at[k, c]).wait()
        blocks = dst.at[c, pl.ds(0, RANKS - 1)]
        pltpu.make_async_copy(blocks, blocks, rsem.at[k, c]).wait()

    def stage_get(first, count, step):
        return jnp.concatenate([stage[b, pl.ds(first, count, stride=step), :] for b in range(8)], axis=1).astype(BF16)

    def stage_put(rows, first, value):
        for b in range(value.shape[1] // 128):
            stage[first + b, rows, :] = value[:, b * 128:b * 128 + 128]

    def regroup(dst, c):
        @pl.loop(0, RANKS, unroll=4)
        def _(p):
            dst[c, p] = stage_get(p, ROWS, RANKS)

    def pipelined(count, scores, probs, mix):
        s, p = {}, {}
        for t in range(count + 2):
            if t < count:
                s[t] = scores(t)
            if 1 <= t <= count:
                p[t - 1] = probs(s.pop(t - 1))
            if t >= 2:
                mix(t - 2, p.pop(t - 2))

    def spatial_attention():
        low = lax.broadcasted_iota(jnp.int32, (64, 128), 1) < 64

        def spread(rows, c0):
            t = qkv[rows, c0:c0 + 256]
            return jnp.concatenate([t, t, t, t], axis=0) * bd_s[...]

        def place(t):
            return slice(t // 4 * 64, t // 4 * 64 + 64), t % 4 * 256

        def scores(t):
            rows, c0 = place(t)
            return dot_nt(qkv[rows, c0:c0 + 256], spread(rows, D + c0))

        def probs(s):
            parts = []
            for side in range(2):
                sc = s[:, side * 128:side * 128 + 128]
                m0 = jnp.max(jnp.where(low, sc, -jnp.inf), axis=-1, keepdims=True)
                m1 = jnp.max(jnp.where(low, -jnp.inf, sc), axis=-1, keepdims=True)
                e = jnp.exp2((sc - jnp.where(low, m0, m1)) * EXP_SCALE)
                d0 = jnp.sum(jnp.where(low, e, 0.0), axis=-1, keepdims=True)
                d1 = jnp.sum(jnp.where(low, 0.0, e), axis=-1, keepdims=True)
                parts.append((e * jnp.where(low, 1.0 / d0, 1.0 / d1)).astype(BF16))
            return jnp.concatenate(parts, axis=1)

        def mix(t, p):
            rows, c0 = place(t)
            o_buf[rows, c0:c0 + 256] = dot(p, spread(rows, 2 * D + c0)).astype(BF16)

        pipelined(16, scores, probs, mix)

    def temporal_attention():
        @pl.loop(0, 4)
        def _(vid):
            rows = pl.ds(pl.multiple_of(vid * 128, 128), 128)

            def spread(c0):
                t = qkv[rows, c0:c0 + 128]
                return jnp.concatenate([t, t], axis=0) * bd_t[...]

            def scores(t):
                return dot_nt(qkv[rows, t * 128:t * 128 + 128], spread(D + t * 128))

            def probs(s):
                parts = []
                for side in range(2):
                    sc = s[:, side * 128:side * 128 + 128]
                    e = jnp.exp2((sc - jnp.max(sc, axis=-1, keepdims=True)) * EXP_SCALE)
                    parts.append((e * (1.0 / jnp.sum(e, axis=-1, keepdims=True))).astype(BF16))
                return jnp.concatenate(parts, axis=1)

            def mix(t, p):
                stage[t, rows, :] = dot(p, spread(2 * D + t * 128)).astype(BF16).astype(F32)

            pipelined(8, scores, probs, mix)

    def spatial_front(i):
        slot = lax.rem(i, 2)
        x_copy(i).wait()

        @pl.when(i + 1 < 2 * GROUPS)
        def _():
            x_copy(i + 1).start()

        g1, s1 = gain[0, 0:1, :], shift[0, 0:1, :]

        for b in range(4):
            rows = slice(b * 64, b * 64 + 64)
            tok = xb[slot, b // 2, b % 2]
            r_buf[rows, :] = tok
            n_buf[rows, :] = normalize(tok.astype(F32), g1, s1).astype(BF16)

        @pl.when(i == 0)
        def _():
            wq0_copy.wait()

        for j in range(6):
            cols = slice(j * 512, j * 512 + 512)
            qkv[0:TILE, cols] = dot_nt(n_buf[0:TILE, :], wq0[cols, :]).astype(BF16)

        spatial_attention()

    def tail_front(i):
        c, half = i // 2, lax.rem(i, 2)

        @pl.when(half == 0)
        def _():
            arrived(or_buf, c, 1)

        @pl.loop(0, 4)
        def _(b):
            rows = pl.ds(pl.multiple_of(b * 64, 64), 64)
            peers = pl.ds(half * 32 + b * 8, 8)
            r_buf[rows, :] = t_buf[c, peers].astype(F32).reshape(64, D).astype(BF16)
            o_buf[rows, :] = or_buf[c, peers].astype(F32).reshape(64, D).astype(BF16)

    def tail(j, base):
        for col in range(2):
            cols = slice(col * 512, col * 512 + 512)
            a = dot(o_buf[...], wo[:, cols]).astype(BF16)
            r_buf[:, cols] = (r_buf[:, cols].astype(F32) + a.astype(F32)).astype(BF16)
        g2, s2 = gain[j, 1:2, :], shift[j, 1:2, :]

        for b in range(4):
            rows = slice(b * 64, b * 64 + 64)
            n_buf[rows, :] = normalize(r_buf[rows, :].astype(F32), g2, s2).astype(BF16)

        prev = None
        for k in range(9):
            cols = slice(k * 512, k * 512 + 512)
            u = dot(n_buf[0:TILE, :], wu[:, cols]).astype(BF16) if k < 8 else None
            if prev is not None:
                g_buf[:, k * 512 - 512:k * 512] = gelu(prev.astype(F32)).astype(BF16)
            prev = u

        for k in range(4):
            cols = slice(k * 256, k * 256 + 256)
            m = dot(g_buf[...], wd[:, cols]).astype(BF16)
            out = (r_buf[:, cols].astype(F32) + m.astype(F32)).astype(BF16)
            stage_put(pl.ds(base, TILE), 2 * k, out.astype(F32))

    def temporal(c):
        arrived(i_buf, c, 0)
        g1, s1 = gain[1, 0:1, :], shift[1, 0:1, :]

        @pl.loop(0, 4)
        def _(b):
            rows = pl.ds(pl.multiple_of(b * 128, 128), 128)
            tok = i_buf[c, pl.ds(b * 16, 16)].astype(F32).reshape(128, D)
            stage_put(rows, 0, normalize(tok, g1, s1))

        for r in range(ROWS):
            n_buf[r * 64:(r + 1) * 64, :] = stage_get(r, RANKS, ROWS)

        @pl.when(c == 0)
        def _():
            wq1_copy.wait()

        for j in range(12):
            cols = slice(j * 256, j * 256 + 256)
            qkv[:, cols] = dot_nt(n_buf[...], wq1[cols, :]).astype(BF16)

        temporal_attention()
        regroup(os_buf, c)
        exchange(os_buf, or_buf, c, 1)

    def tail_back(i):
        half = lax.rem(i, 2)

        @pl.when(i >= 2)
        def _():
            y_copy(i - 2).wait()

        for r in range(ROWS):
            yb[half, r // 2, r % 2] = stage_get(r, 32, ROWS)
        y_copy(i).start()

    @pl.loop(0, 2 * GROUPS)
    def _(step):
        spatial = step < GROUPS

        @pl.loop(0, 2)
        def _(half):
            i = 2 * step + half

            @pl.when(spatial)
            def _():
                spatial_front(i)

            @pl.when(step >= GROUPS)
            def _():
                tail_front(i - 2 * GROUPS)

            @pl.when(jnp.logical_and(half == 0, jnp.logical_or(step == 0, step == GROUPS)))
            def _():
                for copy in weight_copies(0):
                    copy.wait()

            tail(jnp.where(spatial, 0, 1), pl.multiple_of(jnp.where(spatial, half * TILE, 0), TILE))

            @pl.when(step >= GROUPS)
            def _():
                tail_back(i - 2 * GROUPS)

        @pl.when(step == GROUPS - 1)
        def _():
            for copy in weight_copies(1):
                copy.start()

        @pl.when(spatial)
        def _():
            regroup(t_buf, step)
            exchange(t_buf, i_buf, step, 0)

        @pl.when(jnp.logical_and(step >= 1, step <= GROUPS))
        def _():
            temporal(step - 1)

    y_copy(2 * GROUPS - 2).wait()
    y_copy(2 * GROUPS - 1).wait()
    for k, buf in enumerate((t_buf, os_buf)):
        for c in range(GROUPS):
            blocks = buf.at[c, pl.ds(0, RANKS - 1)]
            pltpu.make_async_copy(blocks, blocks, ssem.at[k, c]).wait()


def solution(mesh):
    tok_spec = P(('pod', 'dp'), 'sp', None, None)
    hbm = pl.BlockSpec(memory_space=pl.ANY)
    vmem = pl.BlockSpec(memory_space=pltpu.VMEM)
    comm = pltpu.VMEM((GROUPS, RANKS, ROWS, D), BF16)

    call = pl.pallas_call(
        kernel,
        out_shape=jax.ShapeDtypeStruct((12, 2, 64, D), BF16),
        in_specs=[hbm, vmem, vmem, hbm, hbm, hbm, hbm],
        out_specs=hbm,
        scratch_shapes=[
            pltpu.VMEM((3 * D, D), BF16), pltpu.VMEM((3 * D, D), BF16),
            pltpu.VMEM((D, D), BF16), pltpu.VMEM((D, FF), BF16), pltpu.VMEM((FF, D), BF16),
            pltpu.VMEM((2, 2, 2, 64, D), BF16), pltpu.VMEM((2, 4, 2, 32, D), BF16),
            comm, comm, comm, comm,
            pltpu.VMEM((HALF, D), BF16), pltpu.VMEM((HALF, 3 * D), BF16), pltpu.VMEM((TILE, D), BF16),
            pltpu.VMEM((TILE, D), BF16), pltpu.VMEM((TILE, FF), BF16), pltpu.VMEM((8, HALF, 128), F32),
            pltpu.VMEM((2, 2, D), F32), pltpu.VMEM((2, 2, D), F32),
            pltpu.VMEM((256, 256), BF16), pltpu.VMEM((256, 128), BF16),
            pltpu.SemaphoreType.DMA((5,)), pltpu.SemaphoreType.DMA((2,)), pltpu.SemaphoreType.DMA((2,)),
            pltpu.SemaphoreType.DMA((2, GROUPS)), pltpu.SemaphoreType.DMA((2, GROUPS)),
            pltpu.SemaphoreType.DMA((2, GROUPS)),
        ],
        compiler_params=pltpu.CompilerParams(
            collective_id=0, has_side_effects=True, vmem_limit_bytes=66 * 1000 * 1000),
    )

    def local_step(x_loc, norm_gain, norm_shift, w_qkv, w_out, w_up, w_down):
        w_t = jnp.transpose(w_qkv, (0, 1, 3, 4, 2)).reshape(2, 3 * D, D)
        return call(x_loc, norm_gain, norm_shift, w_t, w_out.reshape(2, D, D), w_up, w_down)

    return jax.shard_map(local_step, mesh=mesh, in_specs=(tok_spec, P(), P(), P(), P(), P(), P()), out_specs=tok_spec, check_vma=False)
```

```python
import jax
import jax.numpy as jnp
from jax import lax
from jax.experimental import pallas as pl
from jax.experimental.pallas import tpu as pltpu
from jax.sharding import PartitionSpec as P

LN_EPS = 1e-6
F32 = jnp.float32
BF16 = jnp.bfloat16
D = 1024
FF = 4096
RANKS = 64
TILES = 6
TILE = 256
ROWS = 8
COLS = 512
SLOTS = 6
SEND_STEP = 23
EXP_SCALE = 0.125 * 1.4426950408889634
GELU_A = 0.7978845608028654
GELU_B = GELU_A * 0.044715
MESH = pl.DeviceIdType.MESH


def dot_nt(a, b):
    return lax.dot_general(a, b, (((1,), (1,)), ((), ())), preferred_element_type=F32)


def dot(a, b):
    return jnp.dot(a, b, preferred_element_type=F32)


def gelu(u):
    half = 0.5 * u
    return half + half * jnp.tanh(u * (GELU_A + GELU_B * (u * u)))


def normalize(tok, gain, shift):
    mean = jnp.mean(tok, axis=-1, keepdims=True)
    cen = tok - mean
    var = jnp.mean(cen * cen, axis=-1, keepdims=True)
    return cen * lax.rsqrt(var + LN_EPS) * gain + shift


def kernel(x_hbm, ng_ref, ns_ref, wqkv_hbm, wo_hbm, wu_hbm, wd_hbm, y_hbm,
           wq, wo, wu, wd, xb, yb, res, t_buf, i_buf, os_buf, or_buf,
           n_a, n_b, qkv, o_a, r_a, o_b, r_b, g_buf, out, s_scr, p_scr,
           gain, shift, bd_s, bd_t, perm, perm_t,
           wsem, xsem, ysem, lsem, ssem, rsem):
    me = lax.axis_index("sp")

    def wq_copy(j):
        return pltpu.make_async_copy(wqkv_hbm.at[j], wq, wsem.at[0])

    def tail_weights(j):
        return (
            pltpu.make_async_copy(wo_hbm.at[j], wo, wsem.at[1]),
            pltpu.make_async_copy(wu_hbm.at[j], wu, wsem.at[2]),
            pltpu.make_async_copy(wd_hbm.at[j], wd, wsem.at[3]),
        )

    def x_copy(i):
        return pltpu.make_async_copy(x_hbm.at[pl.ds(2 * i, 2)], xb.at[lax.rem(i, 2)], xsem.at[lax.rem(i, 2)])

    def y_copy(i):
        return pltpu.make_async_copy(yb.at[lax.rem(i, 2)], y_hbm.at[pl.ds(2 * i, 2)], ysem.at[lax.rem(i, 2)])

    def exchange(src, dst, c, k):
        pltpu.make_async_copy(src.at[c, me], dst.at[c, me], lsem.at[k, c]).start()

        @pl.loop(1, RANKS, unroll=7)
        def _(i):
            peer = lax.rem(me + lax.rem(i * SEND_STEP, RANKS), RANKS)
            pltpu.make_async_remote_copy(
                src_ref=src.at[c, peer], dst_ref=dst.at[c, me], send_sem=ssem.at[k, c], recv_sem=rsem.at[k, c],
                device_id={"sp": peer}, device_id_type=MESH).start()

    def arrived(dst, c, k):
        pltpu.make_async_copy(dst.at[c, 0], dst.at[c, 0], lsem.at[k, c]).wait()
        blocks = dst.at[c, pl.ds(0, RANKS - 1)]
        pltpu.make_async_copy(blocks, blocks, rsem.at[k, c]).wait()

    def regroup(src, dst, c):
        for h in range(2):
            parts = [src[a * 64 + h * 32:a * 64 + h * 32 + 32, n * COLS:n * COLS + COLS] for n in range(2) for a in range(4)]
            moved = dot(perm[...], jnp.concatenate(parts, axis=0))
            dst[c, h * 32:h * 32 + 32] = moved.reshape(32, ROWS, COLS).astype(BF16)

    def ungroup(src, dst, c):
        for h in range(2):
            rows = src[c, h * 32:h * 32 + 32].astype(F32).reshape(TILE, COLS).astype(BF16)
            moved = dot(perm_t[...], rows).astype(BF16)
            for n in range(2):
                for a in range(4):
                    r = (n * 4 + a) * 32
                    dst[a * 64 + h * 32:a * 64 + h * 32 + 32, n * COLS:n * COLS + COLS] = moved[r:r + 32]

    low = lax.broadcasted_iota(jnp.int32, (64, 128), 1) < 64

    def mult(v, m):
        return v if isinstance(v, int) else pl.multiple_of(v, m)

    class Spatial:
        def place(u):
            return pl.ds(mult(u // 4 * 64, 64), 64), mult(u % 4 * 256, 256)

        def spread(rows, c0):
            t = qkv[rows, pl.ds(c0, 256)]
            return jnp.concatenate([t, t, t, t], axis=0) * bd_s[...]

        def scores(u, slot):
            rows, c0 = Spatial.place(u)
            s_scr[slot, 0:64, :] = dot_nt(qkv[rows, pl.ds(c0, 256)], Spatial.spread(rows, D + c0))

        def probs(slot):
            for side in range(2):
                cols = slice(side * 128, side * 128 + 128)
                sc = s_scr[slot, 0:64, cols]
                m0 = jnp.max(jnp.where(low, sc, -jnp.inf), axis=-1, keepdims=True)
                m1 = jnp.max(jnp.where(low, -jnp.inf, sc), axis=-1, keepdims=True)
                e = jnp.exp2((sc - jnp.where(low, m0, m1)) * EXP_SCALE)
                d0 = jnp.sum(jnp.where(low, e, 0.0), axis=-1, keepdims=True)
                d1 = jnp.sum(jnp.where(low, 0.0, e), axis=-1, keepdims=True)
                p_scr[slot, 0:64, cols] = (e * jnp.where(low, 1.0 / d0, 1.0 / d1)).astype(BF16)

        def mix(u, slot):
            rows, c0 = Spatial.place(u)
            o_a[rows, pl.ds(c0, 256)] = dot(p_scr[slot, 0:64, :], Spatial.spread(rows, 2 * D + c0)).astype(BF16)

    class Temporal:
        def place(u):
            return mult(u // 8 * 128, 128), mult(u % 8 * 128, 128)

        def spread(r0, c0):
            t = qkv[pl.ds(r0, 128), pl.ds(c0, 128)]
            return jnp.concatenate([t, t], axis=0) * bd_t[...]

        def scores(u, slot):
            r0, c0 = Temporal.place(u)
            s_scr[slot] = dot_nt(qkv[pl.ds(r0, 128), pl.ds(c0, 128)], Temporal.spread(r0, D + c0))

        def probs(slot):
            for side in range(2):
                cols = slice(side * 128, side * 128 + 128)
                sc = s_scr[slot, :, cols]
                e = jnp.exp2((sc - jnp.max(sc, axis=-1, keepdims=True)) * EXP_SCALE)
                p_scr[slot, :, cols] = (e * (1.0 / jnp.sum(e, axis=-1, keepdims=True))).astype(BF16)

        def mix(u, slot):
            r0, c0 = Temporal.place(u)
            o_a[pl.ds(r0, 128), pl.ds(c0, 128)] = dot(p_scr[slot], Temporal.spread(r0, 2 * D + c0)).astype(BF16)

    def attend(kind, first, count, lo, hi):
        for t in range(lo, hi):
            if 2 <= t < count + 2:
                kind.mix(first + t - 2, (t - 2) % SLOTS)
            if 1 <= t < count + 1:
                kind.probs((t - 1) % SLOTS)
            if t < count:
                kind.scores(first + t, t % SLOTS)

    def spatial_norm(i, b):
        rows = slice(b * 32, b * 32 + 32)
        tok = xb[lax.rem(i, 2), b // 4, b // 2 % 2, b % 2 * 32:b % 2 * 32 + 32, :]
        r_a[rows, :] = tok
        n_a[rows, :] = normalize(tok.astype(F32), gain[0, 0:1, :], shift[0, 0:1, :]).astype(BF16)

    def project(j):
        cols = slice(j * 512, j * 512 + 512)
        qkv[:, cols] = dot_nt(n_a[...], wq[cols, :]).astype(BF16)

    def out_project(j):
        cols = slice(j * 512, j * 512 + 512)
        a = dot(o_b[...], wo[:, cols]).astype(BF16)
        r_b[:, cols] = (r_b[:, cols].astype(F32) + a.astype(F32)).astype(BF16)

    def tail_norm(blk, b):
        rows = slice(b * 32, b * 32 + 32)
        n_b[rows, :] = normalize(r_b[rows, :].astype(F32), gain[blk, 1:2, :], shift[blk, 1:2, :]).astype(BF16)

    def up(k):
        return dot(n_b[...], wu[:, k * 512:k * 512 + 512]).astype(BF16)

    def activate(k, u):
        g_buf[:, k * 512:k * 512 + 512] = gelu(u.astype(F32)).astype(BF16)

    def down(k):
        cols = slice(k * 512, k * 512 + 512)
        m = dot(g_buf[...], wd[:, cols]).astype(BF16)
        out[:, cols] = (r_b[:, cols].astype(F32) + m.astype(F32)).astype(BF16)

    def front_alone(kind):
        if kind is Spatial:
            @pl.loop(0, 3)
            def _(j):
                for q in range(2):
                    cols = pl.ds(pl.multiple_of(j * 1024 + q * 512, 512), 512)
                    qkv[:, cols] = dot_nt(n_a[...], wq[cols, :]).astype(BF16)
        else:
            for j in range(6):
                project(j)

        @pl.loop(0, 2)
        def _(h):
            attend(kind, h * 8, 8, 0, 10)

    def mlp(side):
        prev = None
        for k in range(9):
            u = up(k) if k < 8 else None
            if prev is not None:
                activate(k - 1, prev)
            prev = u
            if k < 8:
                side(k)
        side(8)
        down(0)
        side(9)
        down(1)
        side(10)

    def tail_alone(blk):
        out_project(0)
        out_project(1)
        for b in range(8):
            tail_norm(blk, b)
        mlp(lambda slot: None)

    def both(kind, blk, i):
        for j in range(2):
            out_project(j)
            if kind is Spatial:
                for b in range(4):
                    spatial_norm(i, j * 4 + b)
        for j in range(6):
            project(j)
            if j < 4:
                tail_norm(blk, 2 * j)
                tail_norm(blk, 2 * j + 1)

        @pl.when(i == TILES - 1)
        def _():
            wq_copy(1).start()

        bounds = (0, 1, 2, 3, 4, 5, 6, 7, 8, 11, 15, 18)
        mlp(lambda slot: attend(kind, 0, 16, bounds[slot], bounds[slot + 1]))

    def temporal_front(c):
        arrived(i_buf, c, 0)
        ungroup(i_buf, out, c)
        for b in range(8):
            rows = slice(b * 32, b * 32 + 32)
            n_a[rows, :] = normalize(out[rows, :].astype(F32), gain[1, 0:1, :], shift[1, 0:1, :]).astype(BF16)

    def tail_front(i):
        arrived(or_buf, i, 1)
        ungroup(or_buf, o_b, i)
        for b in range(4):
            rows = slice(b * 64, b * 64 + 64)
            r_b[rows, :] = res[i, rows, :]

    def tail_back(i):
        @pl.when(i >= 2)
        def _():
            y_copy(i - 2).wait()

        for b in range(4):
            yb[lax.rem(i, 2), b // 2, b % 2] = out[b * 64:b * 64 + 64, :]
        y_copy(i).start()

    x_copy(0).start()
    wq_copy(0).start()
    for copy in tail_weights(0):
        copy.start()
    barrier = pltpu.get_barrier_semaphore()

    @pl.loop(1, RANKS)
    def _(i):
        pl.semaphore_signal(barrier, 1, device_id={"sp": lax.rem(me + i, RANKS)}, device_id_type=MESH)

    gain[...] = ng_ref[...].astype(F32)
    shift[...] = ns_ref[...].astype(F32)

    def one_hot(shape, pred):
        row = lax.broadcasted_iota(jnp.int32, shape, 0)
        col = lax.broadcasted_iota(jnp.int32, shape, 1)
        return jnp.where(pred(row, col), 1.0, 0.0).astype(BF16)

    bd_s[...] = one_hot((256, 256), lambda r, c: r // 64 == c // 64)
    bd_t[...] = one_hot((256, 128), lambda r, c: r // 128 == c // 64)
    perm[...] = one_hot((256, 256), lambda r, c: c == r % 8 * 32 + r // 8)
    perm_t[...] = one_hot((256, 256), lambda r, c: c == r % 32 * 8 + r // 32)

    x_copy(0).wait()
    x_copy(1).start()
    for b in range(8):
        spatial_norm(0, b)
    wq_copy(0).wait()
    front_alone(Spatial)
    pl.semaphore_wait(barrier, RANKS - 1)

    @pl.loop(0, 15)
    def _(step):
        last = TILES - 1
        spatial = step <= last
        front = jnp.maximum(step - last, 0)
        tile = jnp.where(spatial, step, jnp.maximum(step - 9, 0))
        has_front = jnp.logical_and(step >= last, step <= 2 * last)
        has_tail = jnp.logical_or(spatial, step >= 9)
        blk = jnp.where(spatial, 0, 1)

        @pl.when(has_front)
        def _():
            temporal_front(front)

        @pl.when(step == last)
        def _():
            wq_copy(1).wait()

        @pl.when(spatial)
        def _():
            for b in range(4):
                rows = slice(b * 64, b * 64 + 64)
                o_b[rows, :] = o_a[rows, :]
                r_b[rows, :] = r_a[rows, :]

        @pl.when(step >= 9)
        def _():
            tail_front(tile)

        @pl.when(jnp.logical_or(step == 0, step == 9))
        def _():
            for copy in tail_weights(0):
                copy.wait()

        @pl.when(step < last)
        def _():
            x_copy(step + 1).wait()

            @pl.when(step + 2 <= last)
            def _():
                x_copy(step + 2).start()

            both(Spatial, 0, step + 1)

        @pl.when(jnp.logical_and(has_front, has_tail))
        def _():
            both(Temporal, blk, 0)

        @pl.when(jnp.logical_and(step > last, step < 9))
        def _():
            front_alone(Temporal)

        @pl.when(step > 2 * last)
        def _():
            tail_alone(1)

        @pl.when(step == last)
        def _():
            for copy in tail_weights(1):
                copy.start()

        @pl.when(spatial)
        def _():
            regroup(out, t_buf, tile)
            exchange(t_buf, i_buf, tile, 0)
            for b in range(4):
                rows = slice(b * 64, b * 64 + 64)
                res[tile, rows, :] = out[rows, :]

        @pl.when(has_front)
        def _():
            regroup(o_a, os_buf, front)
            exchange(os_buf, or_buf, front, 1)

        @pl.when(step >= 9)
        def _():
            tail_back(tile)

    y_copy(TILES - 2).wait()
    y_copy(TILES - 1).wait()
    for k, buf in enumerate((t_buf, os_buf)):
        for c in range(TILES):
            blocks = buf.at[c, pl.ds(0, RANKS - 1)]
            pltpu.make_async_copy(blocks, blocks, ssem.at[k, c]).wait()


def solution(mesh):
    tok_spec = P(('pod', 'dp'), 'sp', None, None)
    hbm = pl.BlockSpec(memory_space=pl.ANY)
    vmem = pl.BlockSpec(memory_space=pltpu.VMEM)
    comm = pltpu.VMEM((TILES, RANKS, ROWS, COLS), BF16)

    def vm(*shape):
        return pltpu.VMEM(shape, BF16)

    call = pl.pallas_call(
        kernel,
        out_shape=jax.ShapeDtypeStruct((12, 2, 64, D), BF16),
        in_specs=[hbm, vmem, vmem, hbm, hbm, hbm, hbm],
        out_specs=hbm,
        scratch_shapes=[
            vm(3 * D, D), vm(D, D), vm(D, FF), vm(FF, D),
            vm(2, 2, 2, 64, D), vm(2, 2, 2, 64, D), vm(TILES, TILE, D), comm, comm, comm, comm,
            vm(TILE, D), vm(TILE, D), vm(TILE, 3 * D), vm(TILE, D), vm(TILE, D), vm(TILE, D), vm(TILE, D),
            vm(TILE, FF), vm(TILE, D), pltpu.VMEM((SLOTS, 128, 256), F32), vm(SLOTS, 128, 256),
            pltpu.VMEM((2, 2, D), F32), pltpu.VMEM((2, 2, D), F32),
            vm(256, 256), vm(256, 128), vm(256, 256), vm(256, 256),
            pltpu.SemaphoreType.DMA((4,)), pltpu.SemaphoreType.DMA((2,)), pltpu.SemaphoreType.DMA((2,)),
            pltpu.SemaphoreType.DMA((2, TILES)), pltpu.SemaphoreType.DMA((2, TILES)),
            pltpu.SemaphoreType.DMA((2, TILES)),
        ],
        compiler_params=pltpu.CompilerParams(
            collective_id=0, has_side_effects=True, vmem_limit_bytes=66 * 1000 * 1000),
    )

    def local_step(x_loc, norm_gain, norm_shift, w_qkv, w_out, w_up, w_down):
        w_t = jnp.transpose(w_qkv, (0, 1, 3, 4, 2)).reshape(2, 3 * D, D)
        return call(x_loc, norm_gain, norm_shift, w_t, w_out.reshape(2, D, D), w_up, w_down)

    return jax.shard_map(local_step, mesh=mesh, in_specs=(tok_spec, P(), P(), P(), P(), P(), P()), out_specs=tok_spec, check_vma=False)
```
